32 devices in a mesh: subj: 8 (over z, y), slab: 4 (over x, core).
Axes of the slice: x: 2, y: 2, z: 4, core: 2. Of those that a mesh axis runs over, the one named last changes fastest.
Arguments:
- fod: bfloat16 [32, 45, 2048], P('subj', None, 'slab'), may hold values from -24 to 24
- rotation: bfloat16 [32, 45, 45, 2048], P('subj', None, None, 'slab'), may hold values from -0.875 to 0.875
- modulation: float32 [32, 2048], P('subj', 'slab'), may hold values from 0.3 to 3
- subject_ids: int32 [32], P('subj'), may hold values from 0 to 31, each once
- subject_weight: float32 [32], replicated, may hold values from 0.5 to 2
- voxel_cell_index: int32 [2048], P('slab'), may hold values from 0 to 1023, as said below
Outputs:
- template: bfloat16 [45, 4096], replicated
The draws below stay inside these ranges and needn't reach their ends.
Inputs may be any that keep to these rules, and one draw needn't show every extreme that they name: `voxel_cell_index`: within each aligned block of 512 entries (one slab's masked voxels) the cell numbers are distinct and increasing.
All inputs are finite; a program needn't handle non-finite values.
Results may differ from the reference program's by a relative error of at most 0.001.
Values may be sent and summed in bfloat16 or wider, within the bound.
A program may use at most 64 MiB of HBM per device.

```python
import math
import jax
import jax.numpy as jnp
from jax import lax

COEF = 45
VOX_DEV = 512
GRID_DEV = 1024
SUBJECTS = 32
MASKED_VOXELS = 2048
N_SLAB = 4


def draw_voxel_cell_index(key, part):
    keys = jax.random.split(jax.random.fold_in(key, 7), N_SLAB)

    def single_slab_block(slab_key):
        order = jax.random.permutation(slab_key, GRID_DEV)
        return jnp.sort(order[:VOX_DEV])
    blocks = jax.vmap(single_slab_block)(keys)
    return blocks.reshape(VOX_DEV * N_SLAB).astype(jnp.int32)


def block_scale(own_key, dims, shards, low, high):
    loudness = 1.0
    for dim, blocks in shards:
        draws = jax.random.uniform(jax.random.fold_in(jax.random.fold_in(own_key, 6), dim), (blocks,), jnp.float32, low / len(shards), high / len(shards))
        loudness = loudness * jnp.repeat(jnp.exp(draws), dims[dim] // blocks).reshape((-1,) + (1,) * (len(dims) - 1 - dim))
    return loudness


def bell_draw(rng, extent, width, bound, shards=(), kind=jnp.bfloat16):
    factor_of = block_scale(rng, extent, shards, -0.22, 0.18) if shards else 1.0
    values = jax.random.normal(rng, extent, jnp.float32) * width * factor_of
    return jnp.minimum(jnp.maximum(values, -bound), bound).astype(kind)


def setup_inputs(seed: int = 0) -> dict:
    seeds = jax.random.split(jax.random.key(seed), 7)
    fod = bell_draw(seeds[0], (SUBJECTS, COEF, MASKED_VOXELS), 4.0, 24.0, ((0, 8), (2, 4)))
    rotation = bell_draw(seeds[1], (SUBJECTS, COEF, COEF, MASKED_VOXELS), COEF ** -0.5, 0.875, ((0, 8), (3, 4)))
    modulation = jnp.clip(jnp.exp(math.log(3.0) - 2.3025851 * jax.random.uniform(seeds[2], (SUBJECTS, MASKED_VOXELS), jnp.float32) ** block_scale(seeds[2], (SUBJECTS, MASKED_VOXELS), ((0, 8), (1, 4)), -0.2, 0.2)), 0.3, 3.0)
    subject_ids = jax.random.permutation(seeds[3], SUBJECTS).astype(jnp.int32)
    subject_weight = jnp.clip(jnp.exp(jax.random.uniform(seeds[4], (SUBJECTS,), jnp.float32, math.log(0.5), math.log(2.0))), 0.5, 2.0)
    voxel_cell_index = draw_voxel_cell_index(jax.random.fold_in(seeds[6], 71), 0)
    return {"fod": fod, "rotation": rotation, "modulation": modulation, "subject_ids": subject_ids, "subject_weight": subject_weight, "voxel_cell_index": voxel_cell_index}


def reference(fod, rotation, modulation, subject_ids, subject_weight, voxel_cell_index):
    selected_cells = subject_weight[subject_ids]
    weight = modulation * selected_cells[:, None]

    def accumulate_weighted(total, items):
        rot_one, fod_one, weight_one = items
        rotated_coefficients = jnp.einsum("ckv,kv->cv", rot_one.astype(jnp.float32), fod_one.astype(jnp.float32))
        return total + rotated_coefficients * weight_one[None, :], None

    start = jnp.zeros((COEF, MASKED_VOXELS), jnp.float32)
    numer, unused = lax.scan(accumulate_weighted, start, (rotation, fod, weight))
    denom = jnp.sum(weight, axis=0)
    average = (numer / denom[None, :]).astype(jnp.bfloat16)
    slab_lookup = (jnp.arange(MASKED_VOXELS, dtype=jnp.int32) // VOX_DEV).astype(jnp.int32)
    cells = (voxel_cell_index + slab_lookup * GRID_DEV).astype(jnp.int32)
    template = jnp.zeros((COEF, GRID_DEV * N_SLAB), jnp.bfloat16)
    return template.at[:, cells].set(average)
```

```python
import functools
import jax
import jax.numpy as jnp
from jax import lax
from jax.experimental import pallas as pl
from jax.experimental.pallas import tpu as pltpu
from jax.sharding import PartitionSpec as P

GRID_DEV = 1024
LANES = 128
SUBLANES = 8
UNROLL = 3
MESH = pl.DeviceIdType.MESH


def near_first(n):
    order = []
    for d in range(1, n // 2 + 1):
        order.append(d)
        if n - d != d:
            order.append(n - d)
    return order


def kernel(n, slabs, groups, rows, fod_h, rot_h, mod_h, ids_ref, sw_ref, cell_h, out_ref,
           fod_v, rot_v, mod_v, cell_v, wf, sums, part, recv, den_part, den_recv, gath, hot,
           in_sem, rot_sem, rs_send, rs_recv, dn_send, dn_recv, ix_send, ix_recv,
           a1_send, a1_recv, a2_send, a2_recv):
    coef, _, height, _ = rot_h.shape
    blocks = cell_h.shape[1] // LANES
    vox = cell_h.shape[1]
    subs = height // blocks
    me = lax.axis_index("subj")
    slab = lax.axis_index("slab")

    fod_in = pltpu.make_async_copy(fod_h, fod_v, in_sem.at[0])
    mod_in = pltpu.make_async_copy(mod_h, mod_v, in_sem.at[1])
    cell_in = pltpu.make_async_copy(cell_h, cell_v.at[slab], in_sem.at[2])
    fod_in.start()
    mod_in.start()
    chunks = []
    for i, c0 in enumerate(range(0, coef, SUBLANES)):
        span = pl.ds(c0, min(SUBLANES, coef - c0))
        chunks.append(pltpu.make_async_copy(rot_h.at[span], rot_v.at[span], rot_sem.at[i]))
        chunks[-1].start()
    cell_in.start()

    barrier = pltpu.get_barrier_semaphore()
    for d in range(1, n):
        pl.semaphore_signal(barrier, inc=1, device_id={"subj": lax.rem(me + d, n)}, device_id_type=MESH)
    for d in range(1, slabs):
        pl.semaphore_signal(barrier, inc=1, device_id={"slab": lax.rem(slab + d, slabs)}, device_id_type=MESH)

    mod_in.wait()
    row = lax.rem(lax.broadcasted_iota(jnp.int32, (height, LANES), 0), subs)
    share = jnp.zeros((height, LANES), jnp.float32)
    for s in range(subs):
        share = jnp.where(row == s, sw_ref[ids_ref[s]], share)
    w = mod_v[...] * share
    for b in range(blocks):
        den_part[b] = jnp.sum(w[b * subs:(b + 1) * subs], axis=0, keepdims=True)
    fod_in.wait()
    wf[...] = fod_v[...].astype(jnp.float32) * w[None]

    def copy_to(src, dst, send, rec, where):
        return pltpu.make_async_remote_copy(
            src_ref=src, dst_ref=dst, send_sem=send, recv_sem=rec,
            device_id=where, device_id_type=MESH)

    def piece_copy(i, g):
        dest = lax.rem(me // groups + i, blocks) * groups + g
        return dest, copy_to(part.at[dest], recv.at[me], rs_send.at[i * groups + g],
                             rs_recv.at[me], {"subj": dest})

    per = rows // SUBLANES
    for g in range(groups):
        for q in range(per):
            base = g * rows + q * SUBLANES
            count = max(0, min(SUBLANES, coef - base))
            if count:
                chunks[base // SUBLANES].wait()

            def step(k, accs):
                factor = wf[k]
                return tuple(acc + rot_v[base + r, k].astype(jnp.float32) * factor
                             for r, acc in enumerate(accs))

            zero = jnp.zeros((height, LANES), jnp.float32)
            if count:
                accs = lax.fori_loop(0, coef, step, (zero,) * count, unroll=UNROLL)
            else:
                accs = ()
            for r in range(SUBLANES):
                sums[q % 2, pl.ds(r * height, height), :] = accs[r] if r < count else zero
            for b in range(blocks):
                tile = None
                for s in range(subs):
                    line = sums[q % 2, pl.ds(b * subs + s, SUBLANES, stride=height), :]
                    tile = line if tile is None else tile + line
                part[b * groups + g, pl.ds(q * SUBLANES, SUBLANES), :] = tile
        if g == 0:
            pl.semaphore_wait(barrier, n + slabs - 2)
        for i in range(blocks):
            dest, copy = piece_copy(i, g)

            @pl.when(dest != me)
            def _():
                copy.start()
        if g == 0:
            for d in range(1, n):
                dest = lax.rem(me + d, n)
                copy_to(den_part.at[dest // groups], den_recv.at[me], dn_send.at[d],
                        dn_recv.at[me], {"subj": dest}).start()
            cell_in.wait()
            for d in range(1, slabs):
                copy_to(cell_v.at[slab], cell_v.at[slab], ix_send.at[d],
                        ix_recv.at[slab], {"slab": lax.rem(slab + d, slabs)}).start()

    def make_hot(p):
        cells = jnp.transpose(jnp.broadcast_to(cell_v[p].astype(jnp.float32), (LANES, vox)))
        lane = lax.broadcasted_iota(jnp.int32, (vox, LANES), 1).astype(jnp.float32)
        for k in range(GRID_DEV // LANES):
            hit = jnp.where(cells == lane + float(k * LANES), 1.0, 0.0)
            hot[p, :, k * LANES:(k + 1) * LANES] = hit.astype(jnp.bfloat16)

    make_hot(slab)

    den = den_part[me // groups]
    for d in near_first(n):
        src = lax.rem(me + d, n)
        copy_to(den_part.at[0], den_recv.at[src], dn_send.at[d], dn_recv.at[src], {"subj": src}).wait_recv()
        den = den + den_recv[src]
    acc = part[me]
    for d in near_first(n):
        src = lax.rem(me + d, n)
        copy_to(part.at[0], recv.at[src], rs_send.at[0], rs_recv.at[src], {"subj": src}).wait_recv()
        acc = acc + recv[src]
    average = (acc / den).reshape(per, SUBLANES, LANES).astype(jnp.bfloat16)
    gath[slab, me] = average

    def forward(d, j):
        peer = lax.rem(slab + d, slabs)
        return copy_to(gath.at[slab, j], gath.at[slab, j], a2_send.at[d, j], a2_recv.at[slab, j],
                       {"slab": peer})

    def first(d):
        return copy_to(gath.at[slab, me], gath.at[slab, me], a1_send.at[d], a1_recv.at[me],
                       {"subj": lax.rem(me + d, n)})

    for d in near_first(n)[::-1]:
        first(d).start()
    for d in range(1, slabs):
        forward(d, me).start()

    for d in range(1, slabs):
        p = lax.rem(slab + d, slabs)
        copy_to(cell_v.at[slab], cell_v.at[p], ix_send.at[d], ix_recv.at[p], {"slab": p}).wait_recv()
        make_hot(p)

    for k in near_first(n):
        src = lax.rem(me + k, n)
        copy_to(gath.at[slab, me], gath.at[slab, src], a1_send.at[k], a1_recv.at[src], {"subj": src}).wait_recv()
        for d in range(1, slabs):
            forward(d, src).start()

    def place(p):
        lines = []
        for g in range(groups):
            cols = [gath[p, b * groups + g].astype(jnp.float32).reshape(rows, LANES) for b in range(blocks)]
            lines.append(jnp.concatenate(cols, axis=1))
        dense = jnp.concatenate(lines, axis=0).astype(jnp.bfloat16)
        placed = jnp.dot(dense, hot[p], preferred_element_type=jnp.float32)
        at = pl.ds(pl.multiple_of(p * GRID_DEV, GRID_DEV), GRID_DEV)
        out_ref[:, at] = placed[:coef].astype(jnp.bfloat16)

    place(slab)
    for d in range(1, slabs):
        p = lax.rem(slab + d, slabs)
        for j in range(n):
            copy_to(gath.at[slab, j], gath.at[p, j], a2_send.at[d, j], a2_recv.at[p, j], {"slab": p}).wait_recv()
        place(p)

    for g in range(groups):
        for i in range(blocks):
            dest, copy = piece_copy(i, g)

            @pl.when(dest != me)
            def _():
                copy.wait_send()
    for d in range(1, n):
        copy_to(den_part.at[0], den_recv.at[me], dn_send.at[d], dn_recv.at[me],
                {"subj": lax.rem(me + d, n)}).wait_send()
        first(d).wait_send()
    for d in range(1, slabs):
        copy_to(cell_v.at[slab], cell_v.at[slab], ix_send.at[d], ix_recv.at[slab],
                {"slab": lax.rem(slab + d, slabs)}).wait_send()
        for j in range(n):
            forward(d, j).wait_send()


def on_device(n, slabs, fod, rotation, modulation, subject_ids, subject_weight, voxel_cell_index):
    subs, coef, _, vox = rotation.shape
    blocks = vox // LANES
    assert vox % LANES == 0 and n % blocks == 0
    groups = n // blocks
    rows = -(-(-(-coef // groups)) // SUBLANES) * SUBLANES
    per = rows // SUBLANES
    height = blocks * subs
    rot_rows = rotation.reshape(subs, coef, coef, blocks, LANES).transpose(1, 2, 3, 0, 4)
    rot_rows = rot_rows.reshape(coef, coef, height, LANES)
    fod_rows = fod.reshape(subs, coef, blocks, LANES).transpose(1, 2, 0, 3).reshape(coef, height, LANES)
    mod_rows = modulation.reshape(subs, blocks, LANES).transpose(1, 0, 2).reshape(height, LANES)
    dma = pltpu.SemaphoreType.DMA
    anywhere = pl.BlockSpec(memory_space=pl.ANY)
    smem = pl.BlockSpec(memory_space=pltpu.SMEM)
    return pl.pallas_call(
        functools.partial(kernel, n, slabs, groups, rows),
        out_shape=jax.ShapeDtypeStruct((coef, slabs * GRID_DEV), jnp.bfloat16),
        in_specs=[anywhere, anywhere, anywhere, smem, smem, anywhere],
        out_specs=pl.BlockSpec(memory_space=pltpu.VMEM),
        scratch_shapes=[
            pltpu.VMEM((coef, height, LANES), jnp.bfloat16),
            pltpu.VMEM((coef, coef, height, LANES), jnp.bfloat16),
            pltpu.VMEM((height, LANES), jnp.float32),
            pltpu.VMEM((slabs, 1, vox), jnp.int32),
            pltpu.VMEM((coef, height, LANES), jnp.float32),
            pltpu.VMEM((2, SUBLANES * height, LANES), jnp.float32),
            pltpu.VMEM((n, rows, LANES), jnp.float32),
            pltpu.VMEM((n, rows, LANES), jnp.float32),
            pltpu.VMEM((blocks, 1, LANES), jnp.float32),
            pltpu.VMEM((n, 1, LANES), jnp.float32),
            pltpu.VMEM((slabs, n, per, SUBLANES, LANES), jnp.bfloat16),
            pltpu.VMEM((slabs, vox, GRID_DEV), jnp.bfloat16),
            dma((3,)),
            dma((-(-coef // SUBLANES),)),
            dma((n,)), dma((n,)),
            dma((n,)), dma((n,)),
            dma((slabs,)), dma((slabs,)),
            dma((n,)), dma((n,)),
            dma((slabs, n)), dma((slabs, n)),
        ],
        compiler_params=pltpu.CompilerParams(collective_id=0, has_side_effects=True),
        name="template",
    )(fod_rows, rot_rows, mod_rows, subject_ids, subject_weight, voxel_cell_index.reshape(1, vox))


def solution(mesh):
    placed = (
        P("subj", None, "slab"),
        P("subj", None, None, "slab"),
        P("subj", "slab"),
        P("subj"),
        P(),
        P("slab"),
    )
    body = functools.partial(on_device, mesh.shape["subj"], mesh.shape["slab"])
    return jax.shard_map(body, mesh=mesh, in_specs=placed, out_specs=P(), check_vma=False)
```

```python
import functools
import jax
import jax.numpy as jnp
from jax import lax
from jax.experimental import pallas as pl
from jax.experimental.pallas import tpu as pltpu
from jax.sharding import PartitionSpec as P

GRID_DEV = 1024
LANES = 128
SUBLANES = 8
UNROLL = 3
AHEAD = 3
MESH = pl.DeviceIdType.MESH


def near_first(n):
    order = []
    for d in range(1, n // 2 + 1):
        order.append(d)
        if n - d != d:
            order.append(n - d)
    return order


def kernel(n, slabs, groups, rows, fod_h, rot_h, mod_h, ids_ref, sw_ref, cell_h, out_ref,
           fod_v, rot_v, mod_v, cell_v, wf, sums, part, recv, den_part, den_recv, gath, hot,
           in_sem, rot_sem, rs_send, rs_recv, dn_send, dn_recv, ix_send, ix_recv,
           a1_send, a1_recv, a2_send, a2_recv):
    coef, _, height, _ = rot_h.shape
    blocks = cell_h.shape[1] // LANES
    vox = cell_h.shape[1]
    subs = height // blocks
    me = lax.axis_index("subj")
    slab = lax.axis_index("slab")

    fod_in = pltpu.make_async_copy(fod_h, fod_v, in_sem.at[0])
    mod_in = pltpu.make_async_copy(mod_h, mod_v, in_sem.at[1])
    cell_in = pltpu.make_async_copy(cell_h, cell_v.at[slab], in_sem.at[2])
    fod_in.start()
    mod_in.start()
    chunks = []
    for i, c0 in enumerate(range(0, coef, SUBLANES)):
        span = pl.ds(c0, min(SUBLANES, coef - c0))
        chunks.append(pltpu.make_async_copy(rot_h.at[span], rot_v.at[span], rot_sem.at[i]))
    for chunk in chunks[:AHEAD]:
        chunk.start()
    cell_in.start()

    barrier = pltpu.get_barrier_semaphore()
    for d in range(1, n):
        pl.semaphore_signal(barrier, inc=1, device_id={"subj": lax.rem(me + d, n)}, device_id_type=MESH)
    for d in range(1, slabs):
        pl.semaphore_signal(barrier, inc=1, device_id={"slab": lax.rem(slab + d, slabs)}, device_id_type=MESH)

    fod_in.wait()
    wf[...] = fod_v[...].astype(jnp.float32)
    mod_in.wait()
    row = lax.rem(lax.broadcasted_iota(jnp.int32, (height, LANES), 0), subs)
    share = jnp.zeros((height, LANES), jnp.float32)
    for s in range(subs):
        share = jnp.where(row == s, sw_ref[ids_ref[s]], share)
    w = mod_v[...] * share
    for b in range(blocks):
        den_part[b] = jnp.sum(w[b * subs:(b + 1) * subs], axis=0, keepdims=True)

    def copy_to(src, dst, send, rec, where):
        return pltpu.make_async_remote_copy(
            src_ref=src, dst_ref=dst, send_sem=send, recv_sem=rec,
            device_id=where, device_id_type=MESH)

    def piece_copy(i, g):
        dest = lax.rem(me // groups + i, blocks) * groups + g
        return dest, copy_to(part.at[dest], recv.at[me], rs_send.at[i * groups + g],
                             rs_recv.at[me], {"subj": dest})

    per = rows // SUBLANES
    for g in range(groups):
        for q in range(per):
            base = g * rows + q * SUBLANES
            count = max(0, min(SUBLANES, coef - base))
            if count:
                here = base // SUBLANES
                chunks[here].wait()
                if here + AHEAD < len(chunks):
                    chunks[here + AHEAD].start()

            def step(k, accs):
                factor = wf[k]
                return tuple(acc + rot_v[base + r, k].astype(jnp.float32) * factor
                             for r, acc in enumerate(accs))

            zero = jnp.zeros((height, LANES), jnp.float32)
            if count:
                accs = lax.fori_loop(0, coef, step, (zero,) * count, unroll=UNROLL)
            else:
                accs = ()
            for r in range(SUBLANES):
                sums[q % 2, pl.ds(r * height, height), :] = accs[r] * w if r < count else zero
            for b in range(blocks):
                tile = None
                for s in range(subs):
                    line = sums[q % 2, pl.ds(b * subs + s, SUBLANES, stride=height), :]
                    tile = line if tile is None else tile + line
                part[b * groups + g, pl.ds(q * SUBLANES, SUBLANES), :] = tile
        if g == 0:
            pl.semaphore_wait(barrier, n + slabs - 2)
        for i in range(blocks):
            dest, copy = piece_copy(i, g)

            @pl.when(dest != me)
            def _():
                copy.start()
        if g == 0:
            for d in range(1, n):
                dest = lax.rem(me + d, n)
                copy_to(den_part.at[dest // groups], den_recv.at[me], dn_send.at[d],
                        dn_recv.at[me], {"subj": dest}).start()
            cell_in.wait()
            for d in range(1, slabs):
                copy_to(cell_v.at[slab], cell_v.at[slab], ix_send.at[d],
                        ix_recv.at[slab], {"slab": lax.rem(slab + d, slabs)}).start()

    def make_hot(p):
        cells = jnp.transpose(jnp.broadcast_to(cell_v[p].astype(jnp.float32), (LANES, vox)))
        lane = lax.broadcasted_iota(jnp.int32, (vox, LANES), 1).astype(jnp.float32)
        for k in range(GRID_DEV // LANES):
            hit = jnp.where(cells == lane + float(k * LANES), 1.0, 0.0)
            hot[p, :, k * LANES:(k + 1) * LANES] = hit.astype(jnp.bfloat16)

    make_hot(slab)
    for d in range(1, slabs):
        p = lax.rem(slab + d, slabs)
        copy_to(cell_v.at[slab], cell_v.at[p], ix_send.at[d], ix_recv.at[p], {"slab": p}).wait_recv()
        make_hot(p)

    den = den_part[me // groups]
    for d in near_first(n):
        src = lax.rem(me + d, n)
        copy_to(den_part.at[0], den_recv.at[src], dn_send.at[d], dn_recv.at[src], {"subj": src}).wait_recv()
        den = den + den_recv[src]
    acc = part[me]
    for d in near_first(n):
        src = lax.rem(me + d, n)
        copy_to(part.at[0], recv.at[src], rs_send.at[0], rs_recv.at[src], {"subj": src}).wait_recv()
        acc = acc + recv[src]
    average = (acc / den).reshape(per, SUBLANES, LANES).astype(jnp.bfloat16)
    gath[slab, me] = average

    half = n // 2
    near = me // half

    def relay(d, side, h):
        rows_of = gath.at[slab, pl.ds(h * half, half)]
        return copy_to(rows_of, rows_of, a2_send.at[d, side], a2_recv.at[slab, h],
                       {"slab": lax.rem(slab + d, slabs)})

    def first(d):
        return copy_to(gath.at[slab, me], gath.at[slab, me], a1_send.at[d], a1_recv.at[me],
                       {"subj": lax.rem(me + d, n)})

    for d in near_first(n)[::-1]:
        first(d).start()

    def arrived(src):
        copy_to(gath.at[slab, me], gath.at[slab, src], a1_send.at[0], a1_recv.at[src], {"subj": src}).wait_recv()

    for k in range(1, half):
        arrived(near * half + lax.rem(me + k, half))
    for d in range(1, slabs):
        relay(d, 0, near).start()
    for k in range(half):
        arrived((1 - near) * half + lax.rem(me + k, half))
    for d in range(1, slabs):
        relay(d, 1, 1 - near).start()

    def place(p):
        lines = []
        for g in range(groups):
            cols = [gath[p, b * groups + g].astype(jnp.float32).reshape(rows, LANES) for b in range(blocks)]
            lines.append(jnp.concatenate(cols, axis=1))
        dense = jnp.concatenate(lines, axis=0).astype(jnp.bfloat16)
        placed = jnp.dot(dense, hot[p], preferred_element_type=jnp.float32)
        at = pl.ds(pl.multiple_of(p * GRID_DEV, GRID_DEV), GRID_DEV)
        out_ref[:, at] = placed[:coef].astype(jnp.bfloat16)

    place(slab)
    for d in range(1, slabs):
        p = lax.rem(slab + d, slabs)
        for h in range(2):
            rows_of = gath.at[p, pl.ds(h * half, half)]
            copy_to(gath.at[slab, pl.ds(0, half)], rows_of, a2_send.at[d, 0], a2_recv.at[p, h], {"slab": p}).wait_recv()
        place(p)

    for g in range(groups):
        for i in range(blocks):
            dest, copy = piece_copy(i, g)

            @pl.when(dest != me)
            def _():
                copy.wait_send()
    for d in range(1, n):
        copy_to(den_part.at[0], den_recv.at[me], dn_send.at[d], dn_recv.at[me],
                {"subj": lax.rem(me + d, n)}).wait_send()
        first(d).wait_send()
    for d in range(1, slabs):
        copy_to(cell_v.at[slab], cell_v.at[slab], ix_send.at[d], ix_recv.at[slab],
                {"slab": lax.rem(slab + d, slabs)}).wait_send()
        relay(d, 0, near).wait_send()
        relay(d, 1, 1 - near).wait_send()


def on_device(n, slabs, fod, rotation, modulation, subject_ids, subject_weight, voxel_cell_index):
    subs, coef, _, vox = rotation.shape
    blocks = vox // LANES
    assert vox % LANES == 0 and n % blocks == 0 and n % 2 == 0
    groups = n // blocks
    rows = -(-(-(-coef // groups)) // SUBLANES) * SUBLANES
    per = rows // SUBLANES
    height = blocks * subs
    rot_rows = rotation.reshape(subs, coef, coef, blocks, LANES).transpose(1, 2, 3, 0, 4)
    rot_rows = rot_rows.reshape(coef, coef, height, LANES)
    fod_rows = fod.reshape(subs, coef, blocks, LANES).transpose(1, 2, 0, 3).reshape(coef, height, LANES)
    mod_rows = modulation.reshape(subs, blocks, LANES).transpose(1, 0, 2).reshape(height, LANES)
    dma = pltpu.SemaphoreType.DMA
    anywhere = pl.BlockSpec(memory_space=pltpu.HBM)
    smem = pl.BlockSpec(memory_space=pltpu.SMEM)
    return pl.pallas_call(
        functools.partial(kernel, n, slabs, groups, rows),
        out_shape=pltpu.VMEM((coef, slabs * GRID_DEV), jnp.bfloat16),
        in_specs=[anywhere, anywhere, anywhere, smem, smem, anywhere],
        out_specs=pl.BlockSpec(memory_space=pltpu.VMEM),
        scratch_shapes=[
            pltpu.VMEM((coef, height, LANES), jnp.bfloat16),
            pltpu.VMEM((coef, coef, height, LANES), jnp.bfloat16),
            pltpu.VMEM((height, LANES), jnp.float32),
            pltpu.VMEM((slabs, 1, vox), jnp.int32),
            pltpu.VMEM((coef, height, LANES), jnp.float32),
            pltpu.VMEM((2, SUBLANES * height, LANES), jnp.float32),
            pltpu.VMEM((n, rows, LANES), jnp.float32),
            pltpu.VMEM((n, rows, LANES), jnp.float32),
            pltpu.VMEM((blocks, 1, LANES), jnp.float32),
            pltpu.VMEM((n, 1, LANES), jnp.float32),
            pltpu.VMEM((slabs, n, per, SUBLANES, LANES), jnp.bfloat16),
            pltpu.VMEM((slabs, vox, GRID_DEV), jnp.bfloat16),
            dma((3,)),
            dma((-(-coef // SUBLANES),)),
            dma((n,)), dma((n,)),
            dma((n,)), dma((n,)),
            dma((slabs,)), dma((slabs,)),
            dma((n,)), dma((n,)),
            dma((slabs, 2)), dma((slabs, 2)),
        ],
        compiler_params=pltpu.CompilerParams(collective_id=0, has_side_effects=True),
        name="template",
    )(fod_rows, rot_rows, mod_rows, subject_ids, subject_weight, voxel_cell_index.reshape(1, vox))


def solution(mesh):
    placed = (
        P("subj", None, "slab"),
        P("subj", None, None, "slab"),
        P("subj", "slab"),
        P("subj"),
        P(),
        P("slab"),
    )
    body = functools.partial(on_device, mesh.shape["subj"], mesh.shape["slab"])
    return jax.shard_map(body, mesh=mesh, in_specs=placed, out_specs=P(), check_vma=False)
```

```python
import functools
import jax
import jax.numpy as jnp
from jax import lax
from jax.experimental import pallas as pl
from jax.experimental.pallas import tpu as pltpu
from jax.sharding import PartitionSpec as P

GRID_DEV = 1024
LANES = 128
SUBLANES = 8
UNROLL = 3
AHEAD = 4
MESH = pl.DeviceIdType.MESH


def near_first(n):
    order = []
    for d in range(1, n // 2 + 1):
        order.append(d)
        if n - d != d:
            order.append(n - d)
    return order


def kernel(n, slabs, groups, rows, fod_h, rot_h, mod_h, ids_h, sw_h, cell_h, out_ref,
           ids_ref, sw_ref, fod_v, rot_v, mod_v, cell_v, wf, sums, part, recv, den_part, den_recv, gath, hot,
           in_sem, rot_sem, rs_send, rs_recv, dn_send, dn_recv, ix_send, ix_recv,
           a1_send, a1_recv, a2_send, a2_recv):
    coef, _, height, _ = rot_h.shape
    blocks = cell_h.shape[1] // LANES
    vox = cell_h.shape[1]
    subs = height // blocks
    me = lax.axis_index("subj")
    slab = lax.axis_index("slab")

    fod_in = pltpu.make_async_copy(fod_h, fod_v, in_sem.at[0])
    mod_in = pltpu.make_async_copy(mod_h, mod_v, in_sem.at[1])
    cell_in = pltpu.make_async_copy(cell_h, cell_v.at[slab], in_sem.at[2])
    fod_in.start()
    mod_in.start()
    ids_in = pltpu.make_async_copy(ids_h, ids_ref, in_sem.at[3])
    sw_in = pltpu.make_async_copy(sw_h, sw_ref, in_sem.at[4])
    ids_in.start()
    sw_in.start()
    chunks = []
    for i, c0 in enumerate(range(0, coef, SUBLANES)):
        span = pl.ds(c0, min(SUBLANES, coef - c0))
        chunks.append(pltpu.make_async_copy(rot_h.at[span], rot_v.at[span], rot_sem.at[i]))
    for chunk in chunks[:AHEAD]:
        chunk.start()
    cell_in.start()

    barrier = pltpu.get_barrier_semaphore()
    for d in range(1, n):
        pl.semaphore_signal(barrier, inc=1, device_id={"subj": lax.rem(me + d, n)}, device_id_type=MESH)
    for d in range(1, slabs):
        pl.semaphore_signal(barrier, inc=1, device_id={"slab": lax.rem(slab + d, slabs)}, device_id_type=MESH)

    fod_in.wait()
    wf[...] = fod_v[...].astype(jnp.float32)
    mod_in.wait()
    ids_in.wait()
    sw_in.wait()
    row = lax.rem(lax.broadcasted_iota(jnp.int32, (height, LANES), 0), subs)
    share = jnp.zeros((height, LANES), jnp.float32)
    for s in range(subs):
        share = jnp.where(row == s, sw_ref[ids_ref[s]], share)
    w = mod_v[...] * share
    for b in range(blocks):
        den_part[b] = jnp.sum(w[b * subs:(b + 1) * subs], axis=0, keepdims=True)

    def copy_to(src, dst, send, rec, where):
        return pltpu.make_async_remote_copy(
            src_ref=src, dst_ref=dst, send_sem=send, recv_sem=rec,
            device_id=where, device_id_type=MESH)

    def piece_copy(i, g):
        dest = lax.rem(me // groups + i, blocks) * groups + g
        return dest, copy_to(part.at[dest], recv.at[me], rs_send.at[i * groups + g],
                             rs_recv.at[me], {"subj": dest})

    per = rows // SUBLANES
    for g in range(groups):
        for q in range(per):
            base = g * rows + q * SUBLANES
            count = max(0, min(SUBLANES, coef - base))
            if count:
                here = base // SUBLANES
                chunks[here].wait()
                if here + AHEAD < len(chunks):
                    chunks[here + AHEAD].start()

            def step(k, accs):
                factor = wf[k]
                return tuple(acc + rot_v[base + r, k].astype(jnp.float32) * factor
                             for r, acc in enumerate(accs))

            zero = jnp.zeros((height, LANES), jnp.float32)
            if count:
                accs = lax.fori_loop(0, coef, step, (zero,) * count, unroll=UNROLL)
            else:
                accs = ()
            for r in range(SUBLANES):
                sums[q % 2, pl.ds(r * height, height), :] = accs[r] * w if r < count else zero
            for b in range(blocks):
                tile = None
                for s in range(subs):
                    line = sums[q % 2, pl.ds(b * subs + s, SUBLANES, stride=height), :]
                    tile = line if tile is None else tile + line
                part[b * groups + g, pl.ds(q * SUBLANES, SUBLANES), :] = tile
        if g == 0:
            pl.semaphore_wait(barrier, n + slabs - 2)
        for i in range(blocks):
            dest, copy = piece_copy(i, g)

            @pl.when(dest != me)
            def _():
                copy.start()
        if g == 0:
            for d in range(1, n):
                dest = lax.rem(me + d, n)
                copy_to(den_part.at[dest // groups], den_recv.at[me], dn_send.at[d],
                        dn_recv.at[me], {"subj": dest}).start()
            cell_in.wait()
            for d in range(1, slabs):
                copy_to(cell_v.at[slab], cell_v.at[slab], ix_send.at[d],
                        ix_recv.at[slab], {"slab": lax.rem(slab + d, slabs)}).start()

    part_vox = vox // 2
    reach = GRID_DEV - part_vox

    def make_hot(p):
        for h in range(2):
            mine = cell_v[p, :, h * part_vox:(h + 1) * part_vox].astype(jnp.float32)
            cells = jnp.transpose(jnp.broadcast_to(mine, (LANES, part_vox)))
            lane = lax.broadcasted_iota(jnp.int32, (part_vox, LANES), 1).astype(jnp.float32)
            for k in range(reach // LANES):
                hit = jnp.where(cells == lane + float(h * part_vox + k * LANES), 1.0, 0.0)
                hot[p, h, :, k * LANES:(k + 1) * LANES] = hit.astype(jnp.bfloat16)

    out_ref[...] = jnp.zeros_like(out_ref)
    pairs = slabs // 2
    peers = [lax.rem(slab // 2 + dp, pairs) * 2 + lax.rem(slab + dc, 2)
             for dp in range(pairs) for dc in range(2)][1:]

    make_hot(slab)
    for p in peers:
        copy_to(cell_v.at[slab], cell_v.at[p], ix_send.at[0], ix_recv.at[p], {"slab": p}).wait_recv()
        make_hot(p)

    den = den_part[me // groups]
    for d in near_first(n):
        src = lax.rem(me + d, n)
        copy_to(den_part.at[0], den_recv.at[src], dn_send.at[d], dn_recv.at[src], {"subj": src}).wait_recv()
        den = den + den_recv[src]
    acc = part[me]
    for d in near_first(n):
        src = lax.rem(me + d, n)
        copy_to(part.at[0], recv.at[src], rs_send.at[0], rs_recv.at[src], {"subj": src}).wait_recv()
        acc = acc + recv[src]
    average = (acc / den).reshape(per, SUBLANES, LANES).astype(jnp.bfloat16)
    gath[slab, me] = average

    half = n // 2
    near = me // half

    quarter = half // 2
    far = 1 - near
    spans = [(near * half, half), (far * half + near * quarter, quarter),
             (far * half + far * quarter, quarter)]

    def relay(i, k):
        start, count = spans[k]
        rows_of = gath.at[slab, pl.ds(start, count)]
        return copy_to(rows_of, rows_of, a2_send.at[i, k], a2_recv.at[slab, k], {"slab": peers[i]})

    def relayed(i, k):
        start, count = spans[k]
        copy_to(gath.at[slab, pl.ds(start, count)], gath.at[peers[i], pl.ds(start, count)],
                a2_send.at[i, k], a2_recv.at[peers[i], k], {"slab": peers[i]}).wait_recv()

    def first(d):
        return copy_to(gath.at[slab, me], gath.at[slab, me], a1_send.at[d], a1_recv.at[me],
                       {"subj": lax.rem(me + d, n)})

    for d in near_first(n)[::-1]:
        first(d).start()

    def arrived(src):
        copy_to(gath.at[slab, me], gath.at[slab, src], a1_send.at[0], a1_recv.at[src], {"subj": src}).wait_recv()

    def place(p, h):
        lines = []
        for g in range(groups):
            cols = [gath[p, h * half + b * groups + g].astype(jnp.float32).reshape(rows, LANES)
                    for b in range(blocks // 2)]
            lines.append(jnp.concatenate(cols, axis=1))
        dense = jnp.concatenate(lines, axis=0).astype(jnp.bfloat16)
        placed = jnp.dot(dense, hot[p, h], preferred_element_type=jnp.float32)
        at = pl.ds(pl.multiple_of(p * GRID_DEV + h * part_vox, LANES), reach)
        held = out_ref[:, at].astype(jnp.float32)
        out_ref[:, at] = (held + placed[:coef]).astype(jnp.bfloat16)

    order = list(range(1, slabs - 1)) + [0]
    for k in range(3):
        start, count = spans[k]
        for i in range(1 if k == 0 else 0, count):
            arrived(near * half + lax.rem(me + i, half) if k == 0 else start + i)
        for i in order:
            relay(i, k).start()
        if k == 0:
            place(slab, near)
    place(slab, far)
    for h, ks in ((near, (0,)), (far, (1, 2))):
        for i in range(slabs - 1):
            for k in ks:
                relayed(i, k)
            place(peers[i], h)

    for g in range(groups):
        for i in range(blocks):
            dest, copy = piece_copy(i, g)

            @pl.when(dest != me)
            def _():
                copy.wait_send()
    for d in range(1, n):
        copy_to(den_part.at[0], den_recv.at[me], dn_send.at[d], dn_recv.at[me],
                {"subj": lax.rem(me + d, n)}).wait_send()
        first(d).wait_send()
    for d in range(1, slabs):
        copy_to(cell_v.at[slab], cell_v.at[slab], ix_send.at[d], ix_recv.at[slab],
                {"slab": lax.rem(slab + d, slabs)}).wait_send()
        for k in range(3):
            relay(d - 1, k).wait_send()


def on_device(n, slabs, fod, rotation, modulation, subject_ids, subject_weight, voxel_cell_index):
    subs, coef, _, vox = rotation.shape
    blocks = vox // LANES
    assert vox % LANES == 0 and n % blocks == 0 and n % 4 == 0 and blocks % 2 == 0 and slabs % 2 == 0
    groups = n // blocks
    rows = -(-(-(-coef // groups)) // SUBLANES) * SUBLANES
    per = rows // SUBLANES
    height = blocks * subs
    rot_rows = rotation.reshape(subs, coef, coef, blocks, LANES).transpose(1, 2, 3, 0, 4)
    rot_rows = rot_rows.reshape(coef, coef, height, LANES)
    fod_rows = fod.reshape(subs, coef, blocks, LANES).transpose(1, 2, 0, 3).reshape(coef, height, LANES)
    mod_rows = modulation.reshape(subs, blocks, LANES).transpose(1, 0, 2).reshape(height, LANES)
    dma = pltpu.SemaphoreType.DMA
    anywhere = pl.BlockSpec(memory_space=pltpu.HBM)
    return pl.pallas_call(
        functools.partial(kernel, n, slabs, groups, rows),
        out_shape=pltpu.VMEM((coef, slabs * GRID_DEV), jnp.bfloat16),
        in_specs=[anywhere] * 6,
        out_specs=pl.BlockSpec(memory_space=pltpu.VMEM),
        scratch_shapes=[
            pltpu.SMEM(subject_ids.shape, jnp.int32),
            pltpu.SMEM(subject_weight.shape, jnp.float32),
            pltpu.VMEM((coef, height, LANES), jnp.bfloat16),
            pltpu.VMEM((coef, coef, height, LANES), jnp.bfloat16),
            pltpu.VMEM((height, LANES), jnp.float32),
            pltpu.VMEM((slabs, 1, vox), jnp.int32),
            pltpu.VMEM((coef, height, LANES), jnp.float32),
            pltpu.VMEM((2, SUBLANES * height, LANES), jnp.float32),
            pltpu.VMEM((n, rows, LANES), jnp.float32),
            pltpu.VMEM((n, rows, LANES), jnp.float32),
            pltpu.VMEM((blocks, 1, LANES), jnp.float32),
            pltpu.VMEM((n, 1, LANES), jnp.float32),
            pltpu.VMEM((slabs, n, per, SUBLANES, LANES), jnp.bfloat16),
            pltpu.VMEM((slabs, 2, vox // 2, GRID_DEV - vox // 2), jnp.bfloat16),
            dma((5,)),
            dma((-(-coef // SUBLANES),)),
            dma((n,)), dma((n,)),
            dma((n,)), dma((n,)),
            dma((slabs,)), dma((slabs,)),
            dma((n,)), dma((n,)),
            dma((slabs, 3)), dma((slabs, 3)),
        ],
        compiler_params=pltpu.CompilerParams(collective_id=0, has_side_effects=True),
        name="template",
    )(fod_rows, rot_rows, mod_rows, subject_ids, subject_weight, voxel_cell_index.reshape(1, vox))


def solution(mesh):
    placed = (
        P("subj", None, "slab"),
        P("subj", None, None, "slab"),
        P("subj", "slab"),
        P("subj"),
        P(),
        P("slab"),
    )
    body = functools.partial(on_device, mesh.shape["subj"], mesh.shape["slab"])
    return jax.shard_map(body, mesh=mesh, in_specs=placed, out_specs=P(), check_vma=False)
```
